32 devices in a mesh: row: 4 (over y, core), col: 8 (over z, x).
Axes of the slice: x: 2, y: 2, z: 4, core: 2. Of those that a mesh axis runs over, the one named last changes fastest.
Arguments:
- density: float32 [4096, 32768], P('row', 'col'), may hold values from 0 to 1
- design_mask: int32 [32, 256], P('row', 'col'), may hold values 0 or 1
- rebalance: int32 [8192], replicated, may hold values from 0 to 8191, as said below
Outputs:
- balanced: bfloat16 [8192, 128, 128], P(('row', 'col'))
- constraint: float32 [], replicated
The draws below stay inside these ranges and needn't reach their ends.
Inputs may be any that keep to these rules, and one draw needn't show every extreme that they name: `rebalance`: A permutation of the 8192 block numbers. Of the blocks that one device holds, the ones that land among one device's output blocks number exactly 8 or none.
All inputs are finite; a program needn't handle non-finite values. No bound on the sum of `design_mask` on one device may be relied on, other than what follows from the above.
Results may differ from the reference program's by a relative error of at most 0.001.
Values may be sent and summed in bfloat16 or wider, within the bound.
A program may use at most 192 MiB of HBM per device.

```python
import jax
import jax.numpy as jnp
from jax import lax

BS = 128
RADIUS = 16
KR = 8
KC = 32
BLOCKS_DEV = 256
CAP = 8
NX = 4096
NY = 32768
NBLK = 8192
N_ROW = 4
N_COL = 8


def draw_rebalance(key, part):
    device_count = N_ROW * N_COL
    group_count = BLOCKS_DEV // CAP
    base = jax.random.fold_in(key, 11)
    key_order, key_offset, key_source, key_target = jax.random.split(base, 4)
    order = jax.random.permutation(key_order, device_count).astype(jnp.int32)
    inverse = jnp.argsort(order).astype(jnp.int32)
    offsets = jax.random.permutation(key_offset, device_count)[:group_count].astype(jnp.int32)
    source_shuffle = jax.vmap(lambda sub: jax.random.permutation(sub, BLOCKS_DEV))(jax.random.split(key_source, device_count)).astype(jnp.int32)
    target_shuffle = jax.vmap(lambda sub: jax.random.permutation(sub, BLOCKS_DEV))(jax.random.split(key_target, device_count)).astype(jnp.int32)
    positions = jnp.arange(NBLK, dtype=jnp.int32)
    target_dev = positions // BLOCKS_DEV
    target_slot = positions % BLOCKS_DEV
    raw_slot = target_shuffle[target_dev, target_slot]
    group = raw_slot // CAP
    within = raw_slot % CAP
    source_dev = (inverse[target_dev] - offsets[group]) % device_count
    local_block = source_shuffle[source_dev, group * CAP + within]
    source_row = source_dev // N_COL
    source_col = source_dev % N_COL
    block_row = source_row * KR + local_block // KC
    block_col = source_col * KC + local_block % KC
    return (block_row * (KC * N_COL) + block_col).astype(jnp.int32)


def set_ends(entries, own_key, smallest, largest):
    place = [jax.random.randint(jax.random.fold_in(own_key, axis), (), 0, length) for axis, length in enumerate(entries.shape)]
    longest = entries.shape.index(max(entries.shape))
    next_to = place[:longest] + [(place[longest] + 1) % entries.shape[longest]] + place[longest + 1:]
    return entries.at[tuple(place)].set(smallest).at[tuple(next_to)].set(largest)


def levels(key, shape, cuts, smallest, high):
    factor_of = 1.0
    for axis_at, shards_of in cuts:
        heights = jax.random.uniform(jax.random.fold_in(jax.random.fold_in(key, 6), axis_at), (shards_of,), jnp.float32, smallest / len(cuts), high / len(cuts))
        factor_of = factor_of * jnp.repeat(jnp.exp(heights), shape[axis_at] // shards_of).reshape((-1,) + (1,) * (len(shape) - 1 - axis_at))
    return factor_of


def setup_inputs(seed: int = 0) -> dict:
    key_list = jax.random.split(jax.random.key(seed), 4)
    return {
        "density": jnp.clip(1.0 * jax.random.uniform(key_list[0], (NX, NY), jnp.float32) ** levels(key_list[0], (NX, NY), ((0, 4), (1, 8)), -0.2, 0.2), 0.0, 1.0),
        "design_mask": set_ends((jax.random.randint(key_list[1], (NX // BS, NY // BS), 0, 4) < 3).astype(jnp.int32), jax.random.fold_in(key_list[1], 1), 0, 1),
        "rebalance": draw_rebalance(jax.random.fold_in(key_list[3], 71), 0),
    }


SHARPNESS = 32.0
THRESHOLD = 0.5
VOLUME_TARGET = 0.4


def filter_taps():
    sigma = RADIUS / 4.0
    offsets = jnp.arange(2 * RADIUS + 1, dtype=jnp.float32) - RADIUS
    raw_taps = jnp.exp(-offsets * offsets / (2.0 * sigma * sigma))
    return raw_taps / jnp.sum(raw_taps)


def smooth(field, weights, axis):
    length = field.shape[axis]
    widths = [(0, 0), (0, 0)]
    widths[axis] = (RADIUS, RADIUS)
    padded = jnp.pad(field, widths)
    total = jnp.zeros_like(field)
    for offset in range(2 * RADIUS + 1):
        total = total + weights[offset] * lax.slice_in_dim(padded, offset, offset + length, axis=axis)
    return total


def reference(density, design_mask, rebalance):
    weights = filter_taps()
    along_rows = smooth(density, weights, 0)
    filtered = smooth(along_rows, weights, 1)
    cell_mask = jnp.repeat(jnp.repeat(design_mask, BS, 0), BS, 1).astype(jnp.float32)
    lower = jnp.tanh(SHARPNESS * THRESHOLD)
    upper = jnp.tanh(SHARPNESS * (1.0 - THRESHOLD))
    projected = cell_mask * (lower + jnp.tanh(SHARPNESS * (filtered - THRESHOLD))) / (lower + upper)
    constraint = jnp.sum(projected) / (NX * NY) / VOLUME_TARGET - 1.0
    block_rows = NX // BS
    block_cols = NY // BS
    tiles = projected.astype(jnp.bfloat16).reshape(block_rows, BS, block_cols, BS)
    tiles = tiles.transpose(0, 2, 1, 3).reshape(block_rows * block_cols, BS, BS)
    balanced = jnp.take(tiles, rebalance.astype(jnp.int32), axis=0)
    return balanced, constraint
```

```python
import functools

import jax
import jax.numpy as jnp
import numpy as np
from jax import lax
from jax.experimental import pallas as pl
from jax.experimental.pallas import tpu as pltpu
from jax.sharding import PartitionSpec as P

BS = 128
RADIUS = 16
SHARPNESS = 32.0
THRESHOLD = 0.5
VOLUME_TARGET = 0.4
MESH = pl.DeviceIdType.MESH
MIB = 2**20


def filter_taps():
    sigma = RADIUS / 4.0
    offsets = np.arange(2 * RADIUS + 1, dtype=np.float64) - RADIUS
    raw_taps = np.exp(-offsets * offsets / (2.0 * sigma * sigma))
    return (raw_taps / raw_taps.sum()).astype(np.float32)


def split(x):
    high = x.astype(jnp.bfloat16)
    return high, (x - high.astype(jnp.float32)).astype(jnp.bfloat16)


def bands():
    taps = filter_taps()
    rows = np.zeros((BS, BS + 2 * RADIUS), np.float32)
    cols = np.zeros((2 * BS, BS), np.float32)
    for out in range(BS):
        for e in range(2 * RADIUS + 1):
            rows[out, out + e] = taps[e]
            source = out + e - RADIUS
            at = source if 0 <= source < BS else BS + source % BS
            cols[at, out] = taps[e]
    return split(jnp.asarray(rows)) + split(jnp.asarray(cols))


def project_block(field, row, col, mask, row_high, row_low, col_high, col_low):
    top = pl.multiple_of(row * BS, BS)
    left = pl.multiple_of(col * BS, BS)
    rows = pl.ds(top, BS + 2 * RADIUS)
    before = field[rows, pl.ds(left, BS)]
    own = field[rows, pl.ds(pl.multiple_of(left + BS, BS), BS)]
    after = field[rows, pl.ds(pl.multiple_of(left + 2 * BS, BS), BS)]
    lane = lax.broadcasted_iota(jnp.int32, own.shape, 1)
    side = jnp.where(lane < BS // 2, after, before)
    high, low = split(jnp.concatenate([own, side], axis=1))
    dot = functools.partial(jnp.dot, preferred_element_type=jnp.float32)
    along = dot(high, col_high[...]) + (dot(low, col_high[...]) + dot(high, col_low[...]))
    high, low = split(along)
    filtered = dot(row_high[...], high) + (dot(row_high[...], low) + dot(row_low[...], high))
    lower = float(np.tanh(np.float32(SHARPNESS * THRESHOLD)))
    upper = float(np.tanh(np.float32(SHARPNESS * (1.0 - THRESHOLD))))
    return (lower + jnp.tanh(SHARPNESS * (filtered - THRESHOLD))) * (mask.astype(jnp.float32) / (lower + upper))


def load_field(field, density, top, bottom, left, right, sem):
    height, width = density.shape
    full = height + 2 * RADIUS
    copies = [
        pltpu.make_async_copy(density, field.at[pl.ds(RADIUS, height), pl.ds(BS, width)], sem.at[0]),
        pltpu.make_async_copy(top, field.at[pl.ds(0, RADIUS), pl.ds(BS, width)], sem.at[1]),
        pltpu.make_async_copy(bottom, field.at[pl.ds(RADIUS + height, RADIUS), pl.ds(BS, width)], sem.at[2]),
        pltpu.make_async_copy(left, field.at[pl.ds(0, full), pl.ds(0, BS)], sem.at[3]),
        pltpu.make_async_copy(right, field.at[pl.ds(0, full), pl.ds(BS + width, BS)], sem.at[4]),
    ]
    for copy in copies:
        copy.start()
    for copy in copies:
        copy.wait()


def halos(density):
    def shift(x, axis, step):
        n = lax.axis_size(axis)
        return lax.ppermute(x, axis, [(i, i + step) for i in range(n) if 0 <= i + step < n])

    top = shift(density[-RADIUS:], "row", 1)
    bottom = shift(density[:RADIUS], "row", -1)
    edges = [
        jnp.concatenate([top[:, cut], density[:, cut], bottom[:, cut]], axis=0)
        for cut in (slice(-RADIUS, None), slice(0, RADIUS))
    ]
    left = jnp.pad(shift(edges[0], "col", 1), ((0, 0), (BS - RADIUS, 0)))
    right = jnp.pad(shift(edges[1], "col", -1), ((0, 0), (0, BS - RADIUS)))
    return top, bottom, left, right


def routing(rebalance, mask_rows, mask_cols, capacity):
    row_count, col_count = lax.axis_size("row"), lax.axis_size("col")
    devices, count = row_count * col_count, mask_rows * mask_cols
    me = lax.axis_index("row") * col_count + lax.axis_index("col")
    wanted = rebalance.reshape(devices, count)
    block_row, block_col = wanted // (mask_cols * col_count), wanted % (mask_cols * col_count)
    source = (block_row // mask_rows) * col_count + block_col // mask_cols
    local = (block_row % mask_rows) * mask_cols + block_col % mask_cols
    slot = jnp.arange(count, dtype=jnp.int32)
    upto = (slot[:, None] <= slot[None, :]).astype(jnp.bfloat16)
    mine = source == me
    seen = jnp.dot(mine.astype(jnp.bfloat16), upto, preferred_element_type=jnp.float32).astype(jnp.int32)
    order = jnp.stack(
        [jnp.sum(jnp.where(mine & (seen == k + 1), local, 0), axis=1) for k in range(capacity)], axis=1
    )
    here = lax.dynamic_slice_in_dim(source, me, 1, axis=0)
    from_each = here == jnp.arange(devices, dtype=jnp.int32)[:, None]
    arrived = jnp.dot(from_each.astype(jnp.bfloat16), upto, preferred_element_type=jnp.float32).astype(jnp.int32)
    slots = jnp.stack(
        [jnp.sum(jnp.where(from_each & (arrived == k + 1), slot[None, :], 0), axis=1) for k in range(capacity)], axis=1
    )
    return order, slots


def place_kernel(groups, slots, arrived, *rest):
    out, held, load_sem, store_sem = rest[-4:]
    size = held.shape[1]

    def load(g):
        return pltpu.make_async_copy(arrived.at[pl.ds(g * size, size)], held.at[g], load_sem.at[g])

    for g in range(groups):
        load(g).start()
    for g in range(groups):
        load(g).wait()
        for i in range(size):
            pltpu.make_async_copy(held.at[g, i], out.at[slots[g * size + i]], store_sem.at[g]).start()
    for g in range(groups):
        pltpu.make_async_copy(held.at[g], out.at[pl.ds(g * size, size)], store_sem.at[g]).wait()


def place(arrived, slots, count, before=None):
    total = arrived.shape[0]
    size = max(s for s in (16, 8, 4, 2, 1) if total % s == 0)
    groups = total // size
    any_space = pl.BlockSpec(memory_space=pl.ANY)
    args = (slots, arrived) + (() if before is None else (before,))
    return pl.pallas_call(
        functools.partial(place_kernel, groups),
        out_shape=jax.ShapeDtypeStruct((count, BS, BS), jnp.bfloat16),
        in_specs=[pl.BlockSpec(memory_space=pltpu.SMEM)] + [any_space] * (len(args) - 1),
        out_specs=any_space,
        scratch_shapes=[
            pltpu.VMEM((groups, size, BS, BS), jnp.bfloat16),
            pltpu.SemaphoreType.DMA((groups,)),
            pltpu.SemaphoreType.DMA((groups,)),
        ],
        input_output_aliases={} if before is None else {2: 0},
        compiler_params=pltpu.CompilerParams(vmem_limit_bytes=24 * MIB),
        cost_estimate=pl.CostEstimate(flops=0, bytes_accessed=2 * arrived.size * 2, transcendentals=0),
        name="place",
    )(*args)


def project_kernel(mask_cols, order, mask, density, top, bottom, left, right, rh, rl, ch, cl, out, total, field, sem):
    @pl.when(pl.program_id(0) == 0)
    def _():
        load_field(field, density, top, bottom, left, right, sem)
        total[...] = jnp.zeros_like(total)

    size = out.shape[0]
    base = pl.program_id(0) * size

    @pl.loop(0, size)
    def _(i):
        block = order[base + i]
        cells = project_block(field, block // mask_cols, block % mask_cols, mask[block], rh, rl, ch, cl)
        total[...] += cells
        out[i] = cells.astype(jnp.bfloat16)


def project(order, mask, mask_cols, density, sides, band):
    count = order.shape[0]
    size = max(s for s in (16, 8, 4, 2, 1) if count % s == 0)
    height, width = density.shape
    any_space = pl.BlockSpec(memory_space=pl.ANY)
    whole = pl.BlockSpec(memory_space=pltpu.VMEM)
    scalar = pl.BlockSpec(memory_space=pltpu.SMEM)
    return pl.pallas_call(
        functools.partial(project_kernel, mask_cols),
        grid=(count // size,),
        out_shape=(
            jax.ShapeDtypeStruct((count, BS, BS), jnp.bfloat16),
            jax.ShapeDtypeStruct((BS, BS), jnp.float32),
        ),
        in_specs=[scalar] * 2 + [any_space] * 5 + [whole] * 4,
        out_specs=(pl.BlockSpec((size, BS, BS), lambda i: (i, 0, 0)), pl.BlockSpec((BS, BS), lambda i: (0, 0))),
        scratch_shapes=[
            pltpu.VMEM((height + 2 * RADIUS, width + 2 * BS), jnp.float32),
            pltpu.SemaphoreType.DMA((5,)),
        ],
        compiler_params=pltpu.CompilerParams(vmem_limit_bytes=40 * MIB, dimension_semantics=("arbitrary",)),
        cost_estimate=pl.CostEstimate(flops=count * BS * BS * 2000, bytes_accessed=density.size * 4, transcendentals=count * BS * BS),
        name="project",
    )(order, mask, density, *sides, *band)


def per_device(density, design_mask, rebalance):
    mask_rows, mask_cols = design_mask.shape
    count = mask_rows * mask_cols
    row_count, col_count = lax.axis_size("row"), lax.axis_size("col")
    devices = row_count * col_count
    capacity = count // devices
    order, slots = routing(rebalance, mask_rows, mask_cols, capacity)
    sides = halos(density)
    mask = design_mask.reshape(count)
    band = bands()
    cuts = sorted({0, max(1, capacity // 8), max(1, capacity // 2), capacity})
    balanced, volume = None, 0.0
    for a, b in zip(cuts[:-1], cuts[1:]):
        blocks, cells = project(order[:, a:b].reshape(-1), mask, mask_cols, density, sides, band)
        volume = volume + cells
        arrived = lax.all_to_all(
            blocks.reshape(devices, b - a, BS, BS), ("row", "col"), split_axis=0, concat_axis=0, tiled=True
        )
        balanced = place(arrived.reshape(-1, BS, BS), slots[:, a:b].reshape(-1), count, balanced)
    total_volume = lax.psum(jnp.sum(volume), ("row", "col"))
    constraint = total_volume / float(density.size * devices) / VOLUME_TARGET - 1.0
    return balanced, constraint


def solution(mesh):
    return jax.shard_map(
        per_device,
        mesh=mesh,
        in_specs=(P("row", "col"), P("row", "col"), P()),
        out_specs=(P(("row", "col"), None, None), P()),
        check_vma=False,
    )
```

```python
import functools

import jax
import jax.numpy as jnp
import numpy as np
from jax import lax
from jax.experimental import pallas as pl
from jax.experimental.pallas import tpu as pltpu
from jax.sharding import PartitionSpec as P

BS = 128
RADIUS = 16
SHARPNESS = 32.0
THRESHOLD = 0.5
VOLUME_TARGET = 0.4
MESH = pl.DeviceIdType.MESH
MIB = 2**20


def filter_taps():
    sigma = RADIUS / 4.0
    offsets = np.arange(2 * RADIUS + 1, dtype=np.float64) - RADIUS
    raw_taps = np.exp(-offsets * offsets / (2.0 * sigma * sigma))
    return (raw_taps / raw_taps.sum()).astype(np.float32)


def split(x):
    high = x.astype(jnp.bfloat16)
    return high, (x - high.astype(jnp.float32)).astype(jnp.bfloat16)


def bands():
    taps = filter_taps()
    rows = np.zeros((BS, BS + 2 * RADIUS), np.float32)
    cols = np.zeros((2 * BS, BS), np.float32)
    for out in range(BS):
        for e in range(2 * RADIUS + 1):
            rows[out, out + e] = taps[e]
            source = out + e - RADIUS
            at = source if 0 <= source < BS else BS + source % BS
            cols[at, out] = taps[e]
    return split(jnp.asarray(rows)) + split(jnp.asarray(cols))


def project_block(before, own, after, mask, row_high, row_low, col_high, col_low):
    lane = lax.broadcasted_iota(jnp.int32, own.shape, 1)
    side = jnp.where(lane < BS // 2, after, before)
    high, low = split(jnp.concatenate([own, side], axis=1))
    dot = functools.partial(jnp.dot, preferred_element_type=jnp.float32)
    along = dot(high, col_high[...]) + (dot(low, col_high[...]) + dot(high, col_low[...]))
    high, low = split(along)
    filtered = dot(row_high[...], high) + (dot(row_high[...], low) + dot(row_low[...], high))
    lower = float(np.tanh(np.float32(SHARPNESS * THRESHOLD)))
    upper = float(np.tanh(np.float32(SHARPNESS * (1.0 - THRESHOLD))))
    return (lower + jnp.tanh(SHARPNESS * (filtered - THRESHOLD))) * (mask.astype(jnp.float32) / (lower + upper))


def load_tiles(tiles, density, top, bottom, left, right, sem):
    height = density.shape[0]
    mask_cols, mask_rows = tiles.shape[0] - 2, tiles.shape[1]
    waits = []

    def begin(source, goal, at):
        copy = pltpu.make_async_copy(source, goal, sem.at[at])
        copy.start()
        waits.append(copy)

    for r in range(mask_rows):
        low, high = max(r * BS - RADIUS, 0), min((r + 1) * BS + RADIUS, height)
        inside = pl.ds(low - (r * BS - RADIUS), high - low)

        @pl.loop(0, mask_cols)
        def _(c):
            cut = density.at[pl.ds(low, high - low), pl.ds(pl.multiple_of(c * BS, BS), BS)]
            pltpu.make_async_copy(cut, tiles.at[c + 1, r, inside], sem.at[r]).start()

        loaded = tiles.at[pl.ds(1, mask_cols), r, inside]
        waits.append(pltpu.make_async_copy(loaded, loaded, sem.at[r]))
        window = pl.ds(r * BS, BS + 2 * RADIUS)
        begin(left.at[window], tiles.at[0, r], mask_rows + r)
        begin(right.at[window], tiles.at[mask_cols + 1, r], 2 * mask_rows + r)
    inner = pl.ds(1, mask_cols)
    begin(top, tiles.at[inner, 0, pl.ds(0, RADIUS)], 3 * mask_rows)
    begin(bottom, tiles.at[inner, mask_rows - 1, pl.ds(BS + RADIUS, RADIUS)], 3 * mask_rows + 1)
    for copy in waits:
        copy.wait()


def halos(density):
    def shift(x, axis, step):
        n = lax.axis_size(axis)
        return lax.ppermute(x, axis, [(i, i + step) for i in range(n) if 0 <= i + step < n])

    top = shift(density[-RADIUS:], "row", 1)
    bottom = shift(density[:RADIUS], "row", -1)
    edges = [
        jnp.concatenate([top[:, cut], density[:, cut], bottom[:, cut]], axis=0)
        for cut in (slice(-RADIUS, None), slice(0, RADIUS))
    ]
    left = jnp.pad(shift(edges[0], "col", 1), ((0, 0), (BS - RADIUS, 0)))
    right = jnp.pad(shift(edges[1], "col", -1), ((0, 0), (0, BS - RADIUS)))
    strips = [x.reshape(RADIUS, -1, BS).transpose(1, 0, 2) for x in (top, bottom)]
    return (*strips, left, right)


def routing(rebalance, mask_rows, mask_cols, capacity):
    row_count, col_count = lax.axis_size("row"), lax.axis_size("col")
    devices, count = row_count * col_count, mask_rows * mask_cols
    me = lax.axis_index("row") * col_count + lax.axis_index("col")
    wanted = rebalance.reshape(devices, count)
    block_row, block_col = wanted // (mask_cols * col_count), wanted % (mask_cols * col_count)
    source = (block_row // mask_rows) * col_count + block_col // mask_cols
    local = (block_row % mask_rows) * mask_cols + block_col % mask_cols
    slot = jnp.arange(count, dtype=jnp.int32)
    upto = (slot[:, None] <= slot[None, :]).astype(jnp.bfloat16)
    mine = source == me
    seen = jnp.dot(mine.astype(jnp.bfloat16), upto, preferred_element_type=jnp.float32).astype(jnp.int32)
    order = jnp.stack(
        [jnp.sum(jnp.where(mine & (seen == k + 1), local, 0), axis=1) for k in range(capacity)], axis=1
    )
    here = lax.dynamic_slice_in_dim(source, me, 1, axis=0)
    from_each = here == jnp.arange(devices, dtype=jnp.int32)[:, None]
    arrived = jnp.dot(from_each.astype(jnp.bfloat16), upto, preferred_element_type=jnp.float32).astype(jnp.int32)
    slots = jnp.stack(
        [jnp.sum(jnp.where(from_each & (arrived == k + 1), slot[None, :], 0), axis=1) for k in range(capacity)], axis=1
    )
    return order, slots


def place_kernel(groups, slots, arrived, *rest):
    out, held, load_sem, store_sem = rest[-4:]
    size = held.shape[1]

    def load(g):
        return pltpu.make_async_copy(arrived.at[pl.ds(g * size, size)], held.at[g], load_sem.at[g])

    for g in range(groups):
        load(g).start()
    for g in range(groups):
        load(g).wait()
        for i in range(size):
            pltpu.make_async_copy(held.at[g, i], out.at[slots[g * size + i]], store_sem.at[g]).start()
    for g in range(groups):
        pltpu.make_async_copy(held.at[g], out.at[pl.ds(g * size, size)], store_sem.at[g]).wait()


def place(arrived, slots, count, before=None):
    total = arrived.shape[0]
    size = max(s for s in (16, 8, 4, 2, 1) if total % s == 0)
    groups = total // size
    any_space = pl.BlockSpec(memory_space=pl.ANY)
    args = (slots, arrived) + (() if before is None else (before,))
    return pl.pallas_call(
        functools.partial(place_kernel, groups),
        out_shape=jax.ShapeDtypeStruct((count, BS, BS), jnp.bfloat16),
        in_specs=[pl.BlockSpec(memory_space=pltpu.SMEM)] + [any_space] * (len(args) - 1),
        out_specs=any_space,
        scratch_shapes=[
            pltpu.VMEM((groups, size, BS, BS), jnp.bfloat16),
            pltpu.SemaphoreType.DMA((groups,)),
            pltpu.SemaphoreType.DMA((groups,)),
        ],
        input_output_aliases={} if before is None else {2: 0},
        compiler_params=pltpu.CompilerParams(vmem_limit_bytes=24 * MIB),
        cost_estimate=pl.CostEstimate(flops=0, bytes_accessed=2 * arrived.size * 2, transcendentals=0),
        name="place",
    )(*args)


def exchange_kernel(
    sizes, block_row, block_col, mask, density, top, bottom, left, right, rh, rl, ch, cl,
    arrived, volume, tiles, outgoing, total, sums, load_sem, send_sem, recv_sem, sum_send, sum_recv,
):
    row_count, col_count = sizes
    devices, capacity = outgoing.shape[:2]
    row, col = lax.axis_index("row"), lax.axis_index("col")
    me = row * col_count + col
    half, quarter = col_count // 2, col_count // 4
    near = quarter * row_count

    def place_of(device):
        return (device // col_count, device % col_count)

    def target(turn):
        early = 1 - turn // (3 * near)
        is_beside = early * (turn % 3 // 2)
        is_across = early - is_beside
        across, beside, close = turn // 3 * 2 + turn % 3, turn // 3, (turn + 1) % near
        far_col = ((col // half + 1) % 2) * half + (col + across) % half
        beside_col = col // half * half + ((col // quarter + 1) % 2) * quarter + (col + beside) % quarter
        close_col = col // quarter * quarter + (col + close) % quarter
        to_col = is_across * far_col + is_beside * beside_col + (1 - early) * close_col
        step = is_across * (across // half) + is_beside * (beside // quarter) + (1 - early) * (close // quarter)
        return (row + step) % row_count * col_count + to_col

    def send(device):
        return pltpu.make_async_remote_copy(
            src_ref=outgoing.at[device], dst_ref=arrived.at[me], send_sem=send_sem.at[device],
            recv_sem=recv_sem.at[me], device_id=place_of(device), device_id_type=MESH,
        )

    def receive(device):
        return pltpu.make_async_remote_copy(
            src_ref=outgoing.at[device], dst_ref=arrived.at[device], send_sem=send_sem.at[device],
            recv_sem=recv_sem.at[device], device_id=place_of(device), device_id_type=MESH,
        )

    def send_sum(device):
        return pltpu.make_async_remote_copy(
            src_ref=sums.at[me], dst_ref=sums.at[me], send_sem=sum_send.at[device],
            recv_sem=sum_recv.at[me], device_id=place_of(device), device_id_type=MESH,
        )

    def receive_sum(device):
        return pltpu.make_async_remote_copy(
            src_ref=sums.at[me], dst_ref=sums.at[device], send_sem=sum_send.at[device],
            recv_sem=sum_recv.at[device], device_id=place_of(device), device_id_type=MESH,
        )

    barrier = pltpu.get_barrier_semaphore()

    @pl.loop(1, devices)
    def _(o):
        pl.semaphore_signal(barrier, inc=1, device_id=place_of((me + o) % devices), device_id_type=MESH)

    load_tiles(tiles, density, top, bottom, left, right, load_sem)
    total[...] = jnp.zeros_like(total)
    pl.semaphore_wait(barrier, devices - 1)

    @pl.loop(0, devices * capacity)
    def _(n):
        turn, k = n // capacity, n % capacity
        device = target(turn)
        at = device * capacity + k
        r, c = block_row[at], block_col[at]
        cells = project_block(tiles[c, r], tiles[c + 1, r], tiles[c + 2, r], mask[at], rh, rl, ch, cl)
        total[...] += cells
        outgoing[device, k] = cells.astype(jnp.bfloat16)

        @pl.when((k == 0) & (turn > 0))
        def _():
            send(target(turn - 1)).start()

    sums[me] = jnp.sum(total[...].reshape(BS // 8, 8, BS), axis=0)
    own = pltpu.make_async_copy(outgoing.at[me], arrived.at[me], load_sem.at[0])
    own.start()
    own.wait()

    @pl.loop(1, devices)
    def _(o):
        send_sum((me + o) % devices).start()

    @pl.loop(1, devices)
    def _(o):
        other = (me + o) % devices
        send_sum(other).wait_send()
        receive_sum(other).wait_recv()

    volume[...] = jnp.sum(sums[...], axis=0)

    @pl.loop(1, devices)
    def _(o):
        other = (me + o) % devices
        send(other).wait_send()
        receive(other).wait_recv()


def exchange(order, mask, mask_cols, density, sides, band, sizes):
    devices, capacity = order.shape
    flat = order.reshape(-1)
    height, width = density.shape
    any_space = pl.BlockSpec(memory_space=pl.ANY)
    whole = pl.BlockSpec(memory_space=pltpu.VMEM)
    scalar = pl.BlockSpec(memory_space=pltpu.SMEM)
    cells = devices * capacity * BS * BS
    return pl.pallas_call(
        functools.partial(exchange_kernel, sizes),
        out_shape=(
            jax.ShapeDtypeStruct((devices, capacity, BS, BS), jnp.bfloat16),
            jax.ShapeDtypeStruct((8, BS), jnp.float32),
        ),
        in_specs=[scalar] * 3 + [any_space] * 5 + [whole] * 4,
        out_specs=(any_space, whole),
        scratch_shapes=[
            pltpu.VMEM((width // BS + 2, height // BS, BS + 2 * RADIUS, BS), jnp.float32),
            pltpu.VMEM((devices, capacity, BS, BS), jnp.bfloat16),
            pltpu.VMEM((BS, BS), jnp.float32),
            pltpu.VMEM((devices, 8, BS), jnp.float32),
            pltpu.SemaphoreType.DMA((3 * (height // BS) + 2,)),
        ]
        + [pltpu.SemaphoreType.DMA((devices,))] * 4,
        compiler_params=pltpu.CompilerParams(vmem_limit_bytes=48 * MIB, collective_id=0, has_side_effects=True),
        cost_estimate=pl.CostEstimate(flops=cells * 2000, bytes_accessed=density.size * 4, transcendentals=cells),
        name="exchange",
    )(flat // mask_cols, flat % mask_cols, mask[flat], density, *sides, *band)


def per_device(density, design_mask, rebalance):
    mask_rows, mask_cols = design_mask.shape
    count = mask_rows * mask_cols
    sizes = (lax.axis_size("row"), lax.axis_size("col"))
    devices = sizes[0] * sizes[1]
    order, slots = routing(rebalance, mask_rows, mask_cols, count // devices)
    arrived, volume = exchange(
        order, design_mask.reshape(count), mask_cols, density, halos(density), bands(), sizes
    )
    constraint = jnp.sum(volume) / float(density.size * devices) / VOLUME_TARGET - 1.0
    balanced = place(arrived.reshape(count, BS, BS), slots.reshape(-1), count)
    return balanced, constraint


def solution(mesh):
    return jax.shard_map(
        per_device,
        mesh=mesh,
        in_specs=(P("row", "col"), P("row", "col"), P()),
        out_specs=(P(("row", "col"), None, None), P()),
        check_vma=False,
    )
```
